512 devices in a mesh: seq: 32 (over x, y), chan: 8 (over z), dp: 2 (over core).
Axes of the slice: x: 4, y: 8, z: 8, core: 2. Of those that a mesh axis runs over, the one named last changes fastest.
Arguments:
- ssm_input: bfloat16 [2, 4096, 4096], P('dp', 'seq', 'chan'), may hold values from -6 to 6
- gate_z: bfloat16 [2, 4096, 4096], P('dp', 'seq', 'chan'), may hold values from -6 to 6
- b_proj: bfloat16 [2, 4096, 128], P('dp', 'seq'), may hold values from -0.52734375 to 0.52734375
- c_proj: bfloat16 [2, 4096, 128], P('dp', 'seq'), may hold values from -6 to 6
- step_size: float32 [2, 4096, 64], P('dp', 'seq', 'chan'), may hold values from 0.02 to 0.2
- log_decay: float32 [2, 4096, 64], P('dp', 'seq', 'chan'), may hold values from -1 to 0, as said below
- skip_d: float32 [64], P('chan'), may hold values from 0.5 to 1.5
- norm_gain: float32 [4096], P('chan'), may hold values from 0.5 to 1.5
- w_out: bfloat16 [4096, 2048], P('chan'), may hold values from -0.09375 to 0.09375
- d_out: bfloat16 [2, 4096, 2048], P('dp', 'seq', 'chan'), may hold values from -6 to 6
- game_lengths: int32 [2, 4], P('dp'), may hold values from 1 to 2048, 4096 in all within a row
Outputs:
- out: bfloat16 [2, 4096, 2048], P('dp', 'seq', 'chan')
- grad_x: bfloat16 [2, 4096, 4096], P('dp', 'seq', 'chan')
- grad_gain: float32 [4096], P('chan')
- grad_skip: float32 [64], P('chan')
The draws below stay inside these ranges and needn't reach their ends.
Inputs may be any that keep to these rules, and one draw needn't show every extreme that they name: `game_lengths`: each row's 4 game lengths sum to 4096, and the longest is exactly 2048. `log_decay`: a log decay per position and head.
All inputs are finite; a program needn't handle non-finite values.
Results may differ from the reference program's by a relative error of at most 0.017.
Values may be sent and summed in bfloat16 or wider, within the bound.
A program may use at most 64 MiB of HBM per device.

```python
import math
import jax
import jax.numpy as jnp
import numpy as np
from jax import lax

D = 2048
MIXER_HEADS = 64
HEADDIM = 64
DSTATE = 128
L_DEV = 128
GAMES = 4
BLOCK = 128
SEQUENCE_LENGTH = 4096
BATCH_SEQUENCES = 2


def draw_log_decay(key, part):
    random_keys = jax.random.split(jax.random.fold_in(key, 71), 7)
    fast_share = 0.5
    fast_pick = jax.random.uniform(random_keys[0], (BATCH_SEQUENCES, 1, MIXER_HEADS), jnp.float32) < fast_share
    fast_rate = jnp.exp(jax.random.uniform(random_keys[1], (BATCH_SEQUENCES, 1, MIXER_HEADS), jnp.float32, jnp.log(0.02), jnp.log(0.035)))
    slow_rate = jnp.exp(jax.random.uniform(random_keys[2], (BATCH_SEQUENCES, 1, MIXER_HEADS), jnp.float32, jnp.log(0.1 / SEQUENCE_LENGTH), jnp.log(0.7 / SEQUENCE_LENGTH)))
    baseline_rate = jnp.where(fast_pick, fast_rate, slow_rate)
    jaggedness = jnp.exp(jax.random.uniform(random_keys[3], (BATCH_SEQUENCES, SEQUENCE_LENGTH, MIXER_HEADS), jnp.float32, -0.7, 0.7))
    worker_level = jnp.exp(jax.random.uniform(random_keys[4], (BATCH_SEQUENCES, SEQUENCE_LENGTH // L_DEV, MIXER_HEADS), jnp.float32, -0.7, 0.7))
    worker_level = jnp.repeat(worker_level, L_DEV, axis=1)
    spike_places = jax.random.randint(random_keys[5], (BATCH_SEQUENCES, 3, MIXER_HEADS), 0, SEQUENCE_LENGTH)
    spike_depth = jax.random.uniform(random_keys[6], (BATCH_SEQUENCES, 3, MIXER_HEADS), jnp.float32, jnp.log(0.5), jnp.log(0.8))
    sequence_positions = jnp.arange(SEQUENCE_LENGTH, dtype=jnp.int32)
    spike_found = sequence_positions[None, :, None, None] == spike_places[:, None, :, :]
    spike_events = jnp.sum(jnp.where(spike_found, spike_depth[:, None, :, :], 0.0), axis=2)
    total = -baseline_rate * jaggedness * worker_level + spike_events
    return jnp.maximum(total, -1.0).astype(jnp.float32)


def shard_levels(key, dims, cuts, low, high):
    level = 1.0
    for dim, parts in cuts:
        draws = jax.random.uniform(jax.random.fold_in(jax.random.fold_in(key, 6), dim), (parts,), jnp.float32, low / len(cuts), high / len(cuts))
        level = level * jnp.repeat(jnp.exp(draws), dims[dim] // parts).reshape((-1,) + (1,) * (len(dims) - 1 - dim))
    return level


def profile(amount, total, reach, slope):
    loads = [(1 << 20) // math.isqrt(grade ** slope) + 1 for grade in range(2, amount + 1)]
    surplus, counts = total - reach - (amount - 1), [1] * (amount - 1)
    while surplus > 0:
        candidates = [i for i in range(amount - 1) if counts[i] < reach]
        pool, left = sum([loads[i] for i in candidates]), surplus
        for i in candidates:
            addition = min(reach - counts[i], max(1, left * loads[i] // pool), surplus)
            counts[i] = counts[i] + addition
            surplus = surplus - addition
    return np.array([reach] + counts)


def ragged(key, count, total, reach, lean):
    if count == 2:
        one = jax.random.randint(key, (), max(1, total - reach), min(reach, total - 1) + 1)
        return jnp.stack([one, total - one])
    tallies = jnp.asarray(profile(count, total, reach, lean), jnp.int32)
    twos = (count - 1) // 2
    source_of, receiver = tallies[1:1 + 2 * twos:2], tallies[2:2 + 2 * twos:2]
    slack = jnp.minimum(source_of - 1, reach - receiver)
    passed = jax.random.randint(jax.random.fold_in(key, 1), (twos,), 0, 1 << 20) % (slack + 1)
    tallies = tallies.at[1:1 + 2 * twos:2].set(source_of - passed).at[2:2 + 2 * twos:2].set(receiver + passed)
    return tallies[jax.random.permutation(jax.random.fold_in(key, 2), count)]


def normal_values(rng, extent, deviation, bound, cuts=(), kind=jnp.bfloat16):
    gain = shard_levels(rng, extent, cuts, -0.22, 0.18) if cuts else 1.0
    entries = jax.random.normal(rng, extent, jnp.float32) * deviation * gain
    return jnp.minimum(jnp.maximum(entries, -bound), bound).astype(kind)


def setup_inputs(seed: int = 0) -> dict:
    seeds = jax.random.split(jax.random.key(seed), 12)
    ssm_input = normal_values(seeds[0], (BATCH_SEQUENCES, SEQUENCE_LENGTH, MIXER_HEADS * HEADDIM), 1.0, 6.0, ((0, 2), (1, 32), (2, 8)))
    gate_z = normal_values(seeds[1], (BATCH_SEQUENCES, SEQUENCE_LENGTH, MIXER_HEADS * HEADDIM), 1.0, 6.0, ((0, 2), (1, 32), (2, 8)))
    b_proj = normal_values(seeds[2], (BATCH_SEQUENCES, SEQUENCE_LENGTH, DSTATE), (DSTATE ** -0.5), 0.52734375, ((0, 2), (1, 32)))
    c_proj = normal_values(seeds[3], (BATCH_SEQUENCES, SEQUENCE_LENGTH, DSTATE), 1.0, 6.0, ((0, 2), (1, 32)))
    step_size = jnp.clip(jnp.exp(math.log(0.2) - 2.3025851 * jax.random.uniform(seeds[4], (BATCH_SEQUENCES, SEQUENCE_LENGTH, MIXER_HEADS), jnp.float32) ** shard_levels(seeds[4], (BATCH_SEQUENCES, SEQUENCE_LENGTH, MIXER_HEADS), ((0, 2), (1, 32), (2, 8)), -0.2, 0.2)), 0.02, 0.2)
    log_decay = draw_log_decay(jax.random.fold_in(seeds[11], 71), 0)
    skip_d = jnp.clip(0.5 + 1.0 * jax.random.uniform(seeds[6], (MIXER_HEADS,), jnp.float32) ** shard_levels(seeds[6], (MIXER_HEADS,), ((0, 8),), -0.2, 0.2), 0.5, 1.5)
    norm_gain = jnp.clip(1.0 + 0.1 * jax.random.normal(seeds[7], (MIXER_HEADS * HEADDIM,), jnp.float32), 0.5, 1.5)
    w_out = normal_values(seeds[8], (MIXER_HEADS * HEADDIM, D), (MIXER_HEADS * HEADDIM) ** -0.5, 0.09375, ((0, 8),))
    d_out = normal_values(seeds[9], (BATCH_SEQUENCES, SEQUENCE_LENGTH, D), 1.0, 6.0, ((0, 2), (1, 32), (2, 8)))
    game_lengths = jax.vmap(lambda own: ragged(own, GAMES, SEQUENCE_LENGTH, SEQUENCE_LENGTH // 2, 2))(jax.random.split(seeds[10], BATCH_SEQUENCES)).reshape((BATCH_SEQUENCES, GAMES)).astype(jnp.int32)
    return dict(ssm_input=ssm_input, gate_z=gate_z, b_proj=b_proj, c_proj=c_proj, step_size=step_size, log_decay=log_decay, skip_d=skip_d, norm_gain=norm_gain, w_out=w_out, d_out=d_out, game_lengths=game_lengths)


NORM_EPS = 1e-05
PRECISE = lax.Precision.HIGHEST

def block_parts(c_block, b_block, dt_block, decay_block, reset_block):
    block_len = c_block.shape[0]
    running = jnp.cumsum(decay_block, axis=0)
    reset_count = jnp.cumsum(reset_block, axis=0).astype(jnp.int32)
    scores = jnp.dot(c_block, b_block.T, preferred_element_type=jnp.float32)
    indices = jnp.arange(block_len, dtype=jnp.int32)
    allowed = (indices[:, None] >= indices[None, :]) & (reset_count[:, None] == reset_count[None, :])
    log_gap = running.T[:, :, None] - running.T[:, None, :]
    mixing = jnp.where(allowed[None], jnp.exp(jnp.minimum(log_gap, 0.0)), 0.0) * scores[None] * dt_block.T[:, None, :]
    mixing = mixing.astype(jnp.bfloat16)
    end_count = reset_count[-1]
    carry_weight = jnp.where((reset_count == 0)[:, None], jnp.exp(running), 0.0)
    tail_weight = jnp.where((reset_count == end_count)[:, None], jnp.exp(running[-1][None, :] - running), 0.0)
    block_decay = jnp.where(end_count == 0, jnp.exp(running[-1]), 0.0)
    return (mixing, carry_weight, tail_weight, block_decay)

def one_sequence(ssm_input, gate_z, b_proj, c_proj, step_size, log_decay, starts, skip_d, norm_gain, w_out, d_out):
    sequence_positions = jnp.arange(SEQUENCE_LENGTH, dtype=jnp.int32)
    resets = jnp.any(sequence_positions[:, None] == starts[None, :], axis=1).astype(jnp.int32)
    count_blocks = SEQUENCE_LENGTH // BLOCK

    def blocked(array):
        return array.reshape((count_blocks, BLOCK) + array.shape[1:])
    x_heads = ssm_input.reshape(SEQUENCE_LENGTH, MIXER_HEADS, HEADDIM)
    zero_state = jnp.zeros((MIXER_HEADS, DSTATE, HEADDIM), jnp.float32)

    def forward_step(state, block_inputs):
        x_block, c_block, b_block, dt_block, decay_block, reset_block = block_inputs
        mixing, carry_weight, tail_weight, block_decay = block_parts(c_block, b_block, dt_block, decay_block, reset_block)
        inside = jnp.einsum('hts,shp->thp', mixing.astype(jnp.float32), x_block.astype(jnp.float32))
        carried = carry_weight[:, :, None] * jnp.einsum('tn,hnp->thp', c_block.astype(jnp.float32), state, precision=PRECISE)
        scaled = ((tail_weight * dt_block)[:, :, None] * x_block.astype(jnp.float32)).astype(jnp.bfloat16)
        fresh_state = jnp.einsum('sn,shp->hnp', b_block.astype(jnp.float32), scaled.astype(jnp.float32))
        return (block_decay[:, None, None] * state + fresh_state, inside + carried)
    _, ssd_blocks = lax.scan(forward_step, zero_state, (blocked(x_heads), blocked(c_proj), blocked(b_proj), blocked(step_size), blocked(log_decay), blocked(resets)))
    ssd_out = ssd_blocks.reshape(SEQUENCE_LENGTH, MIXER_HEADS, HEADDIM) + skip_d[None, :, None] * x_heads.astype(jnp.float32)
    gate_act = jax.nn.silu(gate_z.astype(jnp.float32))
    gated = ssd_out.reshape(SEQUENCE_LENGTH, MIXER_HEADS * HEADDIM) * gate_act
    inv_rms = lax.rsqrt(lax.optimization_barrier(jnp.mean(gated * gated, axis=1)) + NORM_EPS)
    normed = (gated * norm_gain).astype(jnp.bfloat16)
    projected = jnp.dot(normed, w_out, preferred_element_type=jnp.float32)
    out = (inv_rms[:, None] * projected).astype(jnp.bfloat16)
    pulled = jnp.dot(d_out, w_out.T, preferred_element_type=jnp.float32)
    out_dot = lax.optimization_barrier(jnp.sum(d_out.astype(jnp.float32) * projected, axis=1))
    d_normed = inv_rms[:, None] * pulled
    gain_part = lax.optimization_barrier(jnp.sum(gated * d_normed, axis=0))
    d_ssd = ((norm_gain * d_normed - (inv_rms ** 3 * out_dot / (MIXER_HEADS * HEADDIM))[:, None] * gated) * gate_act).astype(jnp.bfloat16)
    d_heads = d_ssd.reshape(SEQUENCE_LENGTH, MIXER_HEADS, HEADDIM)
    skip_part = lax.optimization_barrier(jnp.sum(d_heads.astype(jnp.float32) * x_heads.astype(jnp.float32), axis=(0, 2)))

    def backward_step(adjoint, block_inputs):
        d_block, c_block, b_block, dt_block, decay_block, reset_block = block_inputs
        mixing, carry_weight, tail_weight, block_decay = block_parts(c_block, b_block, dt_block, decay_block, reset_block)
        inside = jnp.einsum('hts,thp->shp', mixing.astype(jnp.float32), d_block.astype(jnp.float32))
        carried = (dt_block * tail_weight)[:, :, None] * jnp.einsum('sn,hnp->shp', b_block.astype(jnp.float32), adjoint, precision=PRECISE)
        weighted = (carry_weight[:, :, None] * d_block.astype(jnp.float32)).astype(jnp.bfloat16)
        fresh_adjoint = jnp.einsum('tn,thp->hnp', c_block.astype(jnp.float32), weighted.astype(jnp.float32))
        return (fresh_adjoint + block_decay[:, None, None] * adjoint, inside + carried)
    _, grad_blocks = lax.scan(backward_step, zero_state, (blocked(d_heads), blocked(c_proj), blocked(b_proj), blocked(step_size), blocked(log_decay), blocked(resets)), reverse=True)
    grad_heads = grad_blocks.reshape(SEQUENCE_LENGTH, MIXER_HEADS, HEADDIM) + skip_d[None, :, None] * d_heads.astype(jnp.float32)
    grad_x = grad_heads.astype(jnp.bfloat16).reshape(SEQUENCE_LENGTH, MIXER_HEADS * HEADDIM)
    return (out, grad_x, gain_part, skip_part)

def reference(ssm_input, gate_z, b_proj, c_proj, step_size, log_decay, skip_d, norm_gain, w_out, d_out, game_lengths):
    outs_list = []
    grads_list = []
    gain_total = jnp.zeros((MIXER_HEADS * HEADDIM,), jnp.float32)
    skip_total = jnp.zeros((MIXER_HEADS,), jnp.float32)
    for index in range(BATCH_SEQUENCES):
        lengths = game_lengths[index].astype(jnp.int32)
        starts = (jnp.cumsum(lengths) - lengths).astype(jnp.int32)
        out, grad_x, gain_part, skip_part = one_sequence(ssm_input[index], gate_z[index], b_proj[index], c_proj[index], step_size[index], log_decay[index], starts, skip_d, norm_gain, w_out, d_out[index])
        outs_list.append(out)
        grads_list.append(grad_x)
        gain_total = gain_total + gain_part
        skip_total = skip_total + skip_part
    return (jnp.stack(outs_list), jnp.stack(grads_list), gain_total, skip_total)
```

```python
import jax
import jax.numpy as jnp
from jax import lax
from jax.experimental import pallas as pl
from jax.experimental.pallas import tpu as pltpu
from jax.sharding import Mesh
from jax.sharding import PartitionSpec as P

SEQ = ("seq_0", "seq_1")
NORM_EPS = 1e-05
MESH = pl.DeviceIdType.MESH
HIGH = lax.Precision.HIGHEST
F32 = jnp.float32
BF16 = jnp.bfloat16


def dot(a, b, ca=1, cb=0, precision=None):
    return lax.dot_general(
        a, b, (((ca,), (cb,)), ((), ())), precision=precision, preferred_element_type=F32
    )


class Exchange:
    def __init__(self, axis, size, source, landing, sends, receives):
        self.axis, self.size, self.me = axis, size, lax.axis_index(axis)
        self.source, self.landing = source, landing
        self.sends, self.receives = sends, receives

    def copy(self, k, slot):
        peer = lax.rem(self.me + k, self.size)
        return pltpu.make_async_remote_copy(
            src_ref=self.source(peer),
            dst_ref=self.landing.at[slot(peer)],
            send_sem=self.sends.at[k - 1],
            recv_sem=self.receives.at[slot(peer)],
            device_id={self.axis: peer},
            device_id_type=MESH,
        )

    def start(self):
        for k in range(1, self.size):
            self.copy(k, lambda peer: self.me).start()

    def receive(self, k):
        self.copy(k, lambda peer: peer).wait_recv()

    def receive_all(self):
        for k in range(1, self.size):
            self.receive(k)

    def finish(self):
        for k in range(1, self.size):
            self.copy(k, lambda peer: self.me).wait_send()


class Shift:
    def __init__(self, axis, size, distance, source, landing, send, receive):
        peer = lax.rem(lax.axis_index(axis) + distance + size, size)
        self.copy = pltpu.make_async_remote_copy(
            src_ref=source,
            dst_ref=landing,
            send_sem=send,
            recv_sem=receive,
            device_id={axis: peer},
            device_id_type=MESH,
        )
        self.start, self.receive, self.finish = (
            self.copy.start,
            self.copy.wait_recv,
            self.copy.wait_send,
        )


def kernel(
    nx,
    ny,
    nz,
    nd,
    length_ref,
    skip_ref,
    x_hbm,
    z_hbm,
    b_hbm,
    c_hbm,
    dt_hbm,
    ld_hbm,
    gain_hbm,
    w_hbm,
    dout_hbm,
    out_ref,
    gx_ref,
    gg_ref,
    gs_ref,
    x_ref,
    z_ref,
    b_ref,
    c_ref,
    dt_ref,
    ld_ref,
    gain_ref,
    w_ref,
    dout_all,
    mix_back,
    decay_all,
    state_out,
    state_in,
    row_state,
    row_in,
    row_decay,
    decay_in,
    back_out,
    back_in,
    adj_out,
    adj_in,
    adj_row,
    adj_row_in,
    adj_back_out,
    adj_back_in,
    stat_all,
    proj_out,
    proj_in,
    sums_y,
    sums_x,
    sums_d,
    load_sem,
    sem_y,
    sem_z,
    sem_x,
    sem_d,
    sem_shift,
):
    length, width = x_ref.shape
    heads = dt_ref.shape[1]
    head_dim = width // heads
    pairs = heads // 2
    lanes = 2 * head_dim
    rows = state_in.shape[1]
    total = width * nz
    me_x, me_y, me_z, me_d = (lax.axis_index(a) for a in ("seq_0", "seq_1", "chan", "dp"))

    loads = {}
    for slot, (name, source, target) in enumerate(
        (
            ("ld", ld_hbm, ld_ref),
            ("dt", dt_hbm, dt_ref),
            ("x", x_hbm, x_ref),
            ("b", b_hbm, b_ref),
            ("dout", dout_hbm, dout_all.at[me_z]),
            ("c", c_hbm, c_ref),
            ("z", z_hbm, z_ref),
            ("gain", gain_hbm, gain_ref),
            ("w", w_hbm, w_ref),
        )
    ):
        loads[name] = pltpu.make_async_copy(source, target, load_sem.at[slot])
        loads[name].start()

    barrier = pltpu.get_barrier_semaphore()
    for axis, size, me in (
        ("seq_1", ny, me_y),
        ("chan", nz, me_z),
        ("seq_0", nx, me_x),
        ("dp", nd, me_d),
    ):
        for k in range(1, size):
            pl.semaphore_signal(
                barrier, inc=1, device_id={axis: lax.rem(me + k, size)}, device_id_type=MESH
            )

    def over_y(index, source, landing):
        return Exchange("seq_1", ny, source, landing, sem_y.at[0, index], sem_y.at[1, index])

    def over_z(index, source, landing):
        return Exchange("chan", nz, source, landing, sem_z.at[0, index], sem_z.at[1, index])

    def shift_x(index, distance, source, landing):
        return Shift(
            "seq_0", nx, distance, source, landing, sem_shift.at[0, index], sem_shift.at[1, index]
        )

    decay_send = over_y(0, lambda peer: decay_all.at[me_y], decay_all)
    state_send = over_y(1, lambda peer: state_out.at[peer], state_in)
    back_send = over_y(2, lambda peer: back_out.at[peer], back_in)
    adj_send = over_y(3, lambda peer: adj_out.at[peer], adj_in)
    adj_back_send = over_y(4, lambda peer: adj_back_out.at[peer], adj_back_in)
    sums_y_send = over_y(5, lambda peer: sums_y.at[me_y], sums_y)
    dout_send = over_z(0, lambda peer: dout_all.at[me_z], dout_all)
    stat_send = over_z(1, lambda peer: stat_all.at[me_z], stat_all)
    proj_send = over_z(2, lambda peer: proj_out.at[peer], proj_in)
    sums_x_send = Exchange(
        "seq_0", nx, lambda peer: sums_x.at[me_x], sums_x, sem_x.at[0], sem_x.at[1]
    )
    sums_d_send = Exchange("dp", nd, lambda peer: sums_d.at[me_d], sums_d, sem_d.at[0], sem_d.at[1])
    row_sends = [shift_x(k, k + 1, row_state, row_in.at[k]) for k in range(2)]
    adj_row_sends = [shift_x(2 + k, -1 - k, adj_row, adj_row_in.at[k]) for k in range(2)]
    decay_sends = [shift_x(4, 1, row_decay, decay_in.at[0]), shift_x(5, -1, row_decay, decay_in.at[1])]

    base = (me_x * ny + me_y) * length
    first = length_ref[0, 0]
    second = first + length_ref[0, 1]
    third = second + length_ref[0, 2]

    def reset_count(position):
        count = jnp.zeros(position.shape, jnp.int32)
        for start in (jnp.int32(0), first, second, third):
            here = jnp.full(position.shape, start - base, jnp.int32)
            count = count + ((here >= 0) & (here <= position)).astype(jnp.int32)
        return count

    at_row = lax.broadcasted_iota(jnp.int32, (length, length), 0)
    at_col = lax.broadcasted_iota(jnp.int32, (length, length), 1)
    count_row = reset_count(at_row)
    count_col = reset_count(at_col)
    count_heads = reset_count(lax.broadcasted_iota(jnp.int32, (length, heads), 0))
    count_end = reset_count(jnp.full((length, heads), length - 1, jnp.int32))
    not_later = (at_row >= at_col).astype(F32)
    spread = (
        lax.broadcasted_iota(jnp.int32, (heads, width), 1) // head_dim
        == lax.broadcasted_iota(jnp.int32, (heads, width), 0)
    ).astype(F32)

    loads["ld"].wait()
    loads["dt"].wait()
    dt = dt_ref[...]
    running = dot(not_later, ld_ref[...], precision=HIGH)
    running_end = running[length - 1 :, :]
    carry_weight = jnp.where(count_heads == 0, jnp.exp(running), 0.0)
    tail_weight = jnp.where(count_heads == count_end, jnp.exp(running_end - running), 0.0)
    block_decay = jnp.where(count_end[:8] == 0, jnp.exp(jnp.broadcast_to(running_end, (8, heads))), 0.0)
    wide = dot(
        jnp.concatenate([tail_weight * dt, carry_weight, block_decay], axis=0), spread, precision=HIGH
    )
    tail_wide, carry_wide = wide[:length], wide[length : 2 * length]
    decay_all[me_y] = wide[2 * length : 2 * length + 1]
    loads["x"].wait()
    loads["b"].wait()
    x = x_ref[...].astype(F32)
    b = b_ref[...]
    fresh = dot(b, (tail_wide * x).astype(BF16), 0, 0).astype(BF16)
    fresh = fresh.reshape(ny, rows, width)
    state_out[...] = fresh
    state_in[me_y] = state_out[me_y]

    pl.semaphore_wait(barrier, (nx - 1) + (ny - 1) + (nz - 1) + (nd - 1))
    decay_send.start()
    state_send.start()
    loads["dout"].wait()
    dout_send.start()

    running_t = dot(ld_ref[...], not_later, 0, 1, precision=HIGH)
    dt_t = dot(dt, (at_row == at_col).astype(F32), 0, 0, precision=HIGH)
    loads["c"].wait()
    c = c_ref[...]
    same_game = count_row == count_col
    scores = jnp.where((at_row >= at_col) & same_game, dot(c, b, 1, 1), 0.0)
    scores_t = jnp.where((at_col >= at_row) & same_game, dot(b, c, 1, 1), 0.0)
    low_lane = lax.broadcasted_iota(jnp.int32, (length, lanes), 1) < head_dim

    def halves(tile):
        return jnp.concatenate([jnp.where(low_lane, tile, 0), jnp.where(low_lane, 0, tile)], axis=0)

    inside = []
    for pair in range(pairs):
        mixes, mixes_t = [], []
        for h in (2 * pair, 2 * pair + 1):
            column = jnp.broadcast_to(running[:, h : h + 1], (length, length))
            line = jnp.broadcast_to(running_t[h : h + 1], (length, length))
            mixes.append(
                (jnp.exp(jnp.minimum(column - line, 0.0)) * scores * dt_t[h : h + 1]).astype(BF16)
            )
            mixes_t.append(
                (jnp.exp(jnp.minimum(line - column, 0.0)) * scores_t * dt[:, h : h + 1]).astype(BF16)
            )
        mix_back[pair] = jnp.concatenate(mixes_t, axis=1)
        tile = x_ref[:, pair * lanes : (pair + 1) * lanes].astype(F32)
        inside.append(dot(jnp.concatenate(mixes, axis=1), halves(tile).astype(BF16)))
    inside = jnp.concatenate(inside, axis=1)
    head_of = lax.broadcasted_iota(jnp.int32, (1, width), 1) // head_dim
    skip = jnp.zeros((1, width), F32)
    for h in range(heads):
        skip = jnp.where(head_of == h, skip_ref[h], skip)
    inside = inside + skip * x
    loads["z"].wait()
    gate = z_ref[...].astype(F32)
    act = gate / (1.0 + jnp.exp(-gate))

    decay_send.receive_all()
    row_product = decay_all[0]
    for k in range(1, ny):
        row_product = row_product * decay_all[k]
    row_decay[...] = row_product
    for shift in decay_sends:
        shift.start()
    state_send.receive_all()
    state = state_in[0].astype(F32)
    for k in range(1, ny):
        state = decay_all[k] * state + state_in[k].astype(F32)
    row_state[...] = state.astype(BF16)
    for shift in row_sends:
        shift.start()
    loads["w"].wait()
    loads["gain"].wait()
    gain = gain_ref[...]
    for shift in decay_sends:
        shift.receive()
    for shift in row_sends:
        shift.receive()
    nearer = jnp.where(me_x >= 1, 1.0, 0.0)
    further = jnp.where(me_x >= 2, 1.0, 0.0)
    state = nearer * row_in[0].astype(F32) + further * (decay_in[0] * row_in[1].astype(F32))
    for k in range(ny):
        back_out[k] = state.astype(BF16)
        if k < ny - 1:
            state = decay_all[k] * state + state_in[k].astype(F32)
    back_in[me_y] = back_out[me_y]
    back_send.start()

    share = dout_all.shape[2]

    def columns(peer):
        return pl.ds(pl.multiple_of(peer * share, share), share)

    pulled = dot(dout_all[me_z], w_ref[:, columns(me_z)], 1, 1)
    for k in range(1, nz):
        dout_send.receive(k)
        peer = lax.rem(me_z + k, nz)
        pulled = pulled + dot(dout_all[peer], w_ref[:, columns(peer)], 1, 1)

    back_send.receive_all()
    from_left = dot(c, back_in[...].reshape(ny * rows, width))
    gated = (inside + carry_wide * from_left) * act
    normed = (gated * gain).astype(BF16)

    def over_features(values):
        part = values[:, :length]
        for k in range(1, width // length):
            part = part + values[:, k * length : (k + 1) * length]
        return jnp.sum(part.T, axis=0, keepdims=True)

    stat_all[me_z] = jnp.concatenate(
        [over_features(gated * gated), over_features(normed.astype(F32) * pulled)], axis=0
    )
    stat_send.start()
    for k in range(1, nz):
        peer = lax.rem(me_z + k, nz)
        proj_out[peer] = dot(normed, w_ref[:, columns(peer)]).astype(BF16)
        proj_send.copy(k, lambda peer: me_z).start()
    projected = dot(normed, w_ref[:, columns(me_z)])
    stat_send.receive_all()
    stats = stat_all[0]
    for k in range(1, nz):
        stats = stats + stat_all[k]
    inv_line = lax.rsqrt(stats[0:1] / total + NORM_EPS)
    pull_line = inv_line * inv_line * inv_line * stats[1:2] / total

    def down(line):
        return jnp.broadcast_to(line, (length, length)).T

    def across(tile):
        return jnp.concatenate([tile] * (width // length), axis=1)

    inv = down(inv_line)
    d_normed = across(inv) * pulled
    d_ssd = ((gain * d_normed - across(down(pull_line)) * gated) * act).astype(BF16)
    d_wide = d_ssd.astype(F32)
    adjoint = dot(c, (carry_wide * d_wide).astype(BF16), 0, 0).astype(BF16)
    adj_out[...] = adjoint.reshape(ny, rows, width)
    adj_in[me_y] = adj_out[me_y]
    adj_send.start()

    gain_part = jnp.sum(gated * d_normed, axis=0, keepdims=True)
    skip_part = jnp.sum(d_wide * x, axis=0, keepdims=True)
    fold = (
        lax.broadcasted_iota(jnp.int32, (width, length), 0) // head_dim
        == lax.broadcasted_iota(jnp.int32, (width, length), 1)
    ).astype(F32)
    skip_part = dot(jnp.broadcast_to(skip_part, (8, width)), fold, precision=HIGH)[:1]
    sums_y[me_y] = jnp.concatenate([gain_part, skip_part], axis=1)
    sums_y_send.start()

    inside_t = []
    for pair in range(pairs):
        tile = d_wide[:, pair * lanes : (pair + 1) * lanes]
        inside_t.append(dot(mix_back[pair], halves(tile).astype(BF16)))
    grad = jnp.concatenate(inside_t, axis=1) + skip * d_wide

    adj_send.receive_all()
    later = adj_in[ny - 1].astype(F32)
    for k in reversed(range(ny - 1)):
        later = decay_all[k] * later + adj_in[k].astype(F32)
    adj_row[...] = later.astype(BF16)
    for shift in adj_row_sends:
        shift.start()

    sums_y_send.receive_all()
    sums = sums_y[0]
    for k in range(1, ny):
        sums = sums + sums_y[k]
    sums_x[me_x] = sums
    sums_x_send.start()

    for shift in adj_row_sends:
        shift.receive()
    nearer = jnp.where(me_x < nx - 1, 1.0, 0.0)
    further = jnp.where(me_x < nx - 2, 1.0, 0.0)
    later = nearer * adj_row_in[0].astype(F32) + further * (decay_in[1] * adj_row_in[1].astype(F32))
    for k in reversed(range(ny)):
        adj_back_out[k] = later.astype(BF16)
        if k > 0:
            later = decay_all[k] * later + adj_in[k].astype(F32)
    adj_back_in[me_y] = adj_back_out[me_y]
    adj_back_send.start()

    sums_x_send.receive_all()
    sums = sums_x[0]
    for k in range(1, nx):
        sums = sums + sums_x[k]
    sums_d[me_d] = sums
    sums_d_send.start()

    for k in range(1, nz):
        proj_send.receive(k)
        projected = projected + proj_in[lax.rem(me_z + k, nz)].astype(F32)
    out_ref[...] = (jnp.concatenate([inv] * (share // length), axis=1) * projected).astype(BF16)

    sums_d_send.receive_all()
    sums = sums_d[0] + sums_d[1]
    gg_ref[...] = sums[:, :width]
    gs_ref[...] = sums[:, width:]

    adj_back_send.receive_all()
    right = dot(b, adj_back_in[...].reshape(ny * rows, width))
    gx_ref[...] = (grad + tail_wide * right).astype(BF16)

    for sent in (
        decay_send,
        state_send,
        back_send,
        adj_send,
        adj_back_send,
        sums_y_send,
        dout_send,
        stat_send,
        proj_send,
        sums_x_send,
        sums_d_send,
        *row_sends,
        *adj_row_sends,
        *decay_sends,
    ):
        sent.finish()


def mixer(
    sizes,
    ssm_input,
    gate_z,
    b_proj,
    c_proj,
    step_size,
    log_decay,
    skip_d,
    norm_gain,
    w_out,
    d_out,
    game_lengths,
):
    nx, ny, nz, nd = sizes
    length, width = ssm_input.shape[1:]
    heads = step_size.shape[2]
    state_dim = b_proj.shape[2]
    share = d_out.shape[2]
    rows = state_dim // ny
    pack = width + length

    def body(*refs):
        return kernel(nx, ny, nz, nd, *refs)

    hbm = pl.BlockSpec(memory_space=pltpu.HBM)
    smem = pl.BlockSpec(memory_space=pltpu.SMEM)
    vmem = pl.BlockSpec(memory_space=pltpu.VMEM)
    dma = pltpu.SemaphoreType.DMA
    out, grad_x, gain_sum, skip_sum = pl.pallas_call(
        body,
        out_shape=(
            jax.ShapeDtypeStruct((length, share), BF16),
            jax.ShapeDtypeStruct((length, width), BF16),
            jax.ShapeDtypeStruct((1, width), F32),
            jax.ShapeDtypeStruct((1, length), F32),
        ),
        in_specs=[smem, smem] + [hbm] * 9,
        out_specs=(vmem, vmem, vmem, vmem),
        scratch_shapes=[
            pltpu.VMEM((length, width), BF16),
            pltpu.VMEM((length, width), BF16),
            pltpu.VMEM((length, state_dim), BF16),
            pltpu.VMEM((length, state_dim), BF16),
            pltpu.VMEM((length, heads), F32),
            pltpu.VMEM((length, heads), F32),
            pltpu.VMEM((1, width), F32),
            pltpu.VMEM(w_out.shape, BF16),
            pltpu.VMEM((nz, length, share), BF16),
            pltpu.VMEM((heads // 2, length, 2 * length), BF16),
            pltpu.VMEM((ny, 1, width), F32),
            pltpu.VMEM((ny, rows, width), BF16),
            pltpu.VMEM((ny, rows, width), BF16),
            pltpu.VMEM((rows, width), BF16),
            pltpu.VMEM((2, rows, width), BF16),
            pltpu.VMEM((1, width), F32),
            pltpu.VMEM((2, 1, width), F32),
            pltpu.VMEM((ny, rows, width), BF16),
            pltpu.VMEM((ny, rows, width), BF16),
            pltpu.VMEM((ny, rows, width), BF16),
            pltpu.VMEM((ny, rows, width), BF16),
            pltpu.VMEM((rows, width), BF16),
            pltpu.VMEM((2, rows, width), BF16),
            pltpu.VMEM((ny, rows, width), BF16),
            pltpu.VMEM((ny, rows, width), BF16),
            pltpu.VMEM((nz, 2, length), F32),
            pltpu.VMEM((nz, length, share), BF16),
            pltpu.VMEM((nz, length, share), BF16),
            pltpu.VMEM((ny, 1, pack), F32),
            pltpu.VMEM((nx, 1, pack), F32),
            pltpu.VMEM((nd, 1, pack), F32),
            dma((9,)),
            dma((2, 6, ny)),
            dma((2, 3, nz)),
            dma((2, nx)),
            dma((2, nd)),
            dma((2, 6)),
        ],
        compiler_params=pltpu.CompilerParams(
            collective_id=0, has_side_effects=True, vmem_limit_bytes=48 * 1024 * 1024
        ),
        name="mixer",
    )(
        game_lengths,
        skip_d,
        ssm_input[0],
        gate_z[0],
        b_proj[0],
        c_proj[0],
        step_size[0],
        log_decay[0],
        norm_gain[None],
        w_out,
        d_out[0],
    )
    return (out[None], grad_x[None], gain_sum[0], skip_sum[0, :heads])


def solution(mesh):
    nz, nd = mesh.shape["chan"], mesh.shape["dp"]
    ny = 8
    nx = mesh.shape["seq"] // ny
    finer = Mesh(mesh.devices.reshape(nx, ny, nz, nd), ("seq_0", "seq_1", "chan", "dp"))

    def local(*args):
        return mixer((nx, ny, nz, nd), *args)

    return jax.shard_map(
        local,
        mesh=finer,
        in_specs=(
            P("dp", SEQ, "chan"),
            P("dp", SEQ, "chan"),
            P("dp", SEQ, None),
            P("dp", SEQ, None),
            P("dp", SEQ, "chan"),
            P("dp", SEQ, "chan"),
            P("chan"),
            P("chan"),
            P("chan", None),
            P("dp", SEQ, "chan"),
            P("dp", None),
        ),
        out_specs=(P("dp", SEQ, "chan"), P("dp", SEQ, "chan"), P("chan"), P("chan")),
        check_vma=False,
    )
```

```python
import jax
import jax.numpy as jnp
from jax import lax
from jax.experimental import pallas as pl
from jax.experimental.pallas import tpu as pltpu
from jax.sharding import Mesh
from jax.sharding import PartitionSpec as P

SEQ = ("seq_0", "seq_1")
NORM_EPS = 1e-05
VMEM_LIMIT = 48 * 1024 * 1024
MESH = pl.DeviceIdType.MESH
HIGH = lax.Precision.HIGHEST
F32 = jnp.float32
BF16 = jnp.bfloat16


def dot(a, b, ca=1, cb=0, precision=None):
    return lax.dot_general(
        a, b, (((ca,), (cb,)), ((), ())), precision=precision, preferred_element_type=F32
    )


class Exchange:
    def __init__(self, axis, size, source, landing, sends, receives):
        self.axis, self.size, self.me = axis, size, lax.axis_index(axis)
        self.source, self.landing = source, landing
        self.sends, self.receives = sends, receives

    def copy(self, k, slot):
        peer = lax.rem(self.me + k, self.size)
        return pltpu.make_async_remote_copy(
            src_ref=self.source(peer),
            dst_ref=self.landing.at[slot(peer)],
            send_sem=self.sends.at[k - 1],
            recv_sem=self.receives.at[slot(peer)],
            device_id={self.axis: peer},
            device_id_type=MESH,
        )

    def start(self):
        for k in range(1, self.size):
            self.copy(k, lambda peer: self.me).start()

    def receive(self, k):
        self.copy(k, lambda peer: peer).wait_recv()

    def receive_all(self):
        for k in range(1, self.size):
            self.receive(k)

    def finish(self):
        for k in range(1, self.size):
            self.copy(k, lambda peer: self.me).wait_send()


class Shift:
    def __init__(self, axis, size, distance, source, landing, send, receive):
        peer = lax.rem(lax.axis_index(axis) + distance + size, size)
        self.copy = pltpu.make_async_remote_copy(
            src_ref=source,
            dst_ref=landing,
            send_sem=send,
            recv_sem=receive,
            device_id={axis: peer},
            device_id_type=MESH,
        )
        self.start, self.receive, self.finish = (
            self.copy.start,
            self.copy.wait_recv,
            self.copy.wait_send,
        )


def kernel(
    nx,
    ny,
    nz,
    nd,
    length_hbm,
    skip_hbm,
    x_hbm,
    z_hbm,
    b_hbm,
    c_hbm,
    dt_hbm,
    ld_hbm,
    gain_hbm,
    w_hbm,
    dout_hbm,
    out_ref,
    gx_ref,
    gg_ref,
    gs_ref,
    length_ref,
    skip_ref,
    x_ref,
    z_ref,
    b_ref,
    c_ref,
    dt_ref,
    ld_ref,
    gain_ref,
    w_ref,
    dout_all,
    mix_back,
    decay_all,
    state_out,
    state_in,
    row_state,
    row_in,
    row_decay,
    decay_in,
    back_out,
    back_in,
    adj_out,
    adj_in,
    adj_row,
    adj_row_in,
    adj_back_out,
    adj_back_in,
    stat_all,
    proj_out,
    proj_in,
    sums_y,
    sums_x,
    sums_d,
    load_sem,
    sem_y,
    sem_z,
    sem_x,
    sem_d,
    sem_shift,
):
    length, width = x_ref.shape
    heads = dt_ref.shape[0]
    head_dim = width // heads
    pairs = heads // 2
    lanes = 2 * head_dim
    rows = state_in.shape[1]
    total = width * nz
    me_x, me_y, me_z, me_d = (lax.axis_index(a) for a in ("seq_0", "seq_1", "chan", "dp"))

    loads = {}
    for slot, (name, source, target) in enumerate(
        (
            ("length", length_hbm, length_ref),
            ("ld", ld_hbm, ld_ref),
            ("dt", dt_hbm, dt_ref),
            ("x", x_hbm, x_ref),
            ("b", b_hbm, b_ref),
            ("dout", dout_hbm, dout_all.at[me_z]),
            ("c", c_hbm, c_ref),
            ("z", z_hbm, z_ref),
            ("gain", gain_hbm, gain_ref),
            ("skip", skip_hbm, skip_ref),
            ("w", w_hbm, w_ref),
        )
    ):
        loads[name] = pltpu.make_async_copy(source, target, load_sem.at[slot])
        loads[name].start()

    barrier = pltpu.get_barrier_semaphore()
    for axis, size, me in (
        ("seq_1", ny, me_y),
        ("chan", nz, me_z),
        ("seq_0", nx, me_x),
        ("dp", nd, me_d),
    ):
        for k in range(1, size):
            pl.semaphore_signal(
                barrier, inc=1, device_id={axis: lax.rem(me + k, size)}, device_id_type=MESH
            )

    def over_y(index, source, landing):
        return Exchange("seq_1", ny, source, landing, sem_y.at[0, index], sem_y.at[1, index])

    def over_z(index, source, landing):
        return Exchange("chan", nz, source, landing, sem_z.at[0, index], sem_z.at[1, index])

    def shift_x(index, distance, source, landing):
        return Shift(
            "seq_0", nx, distance, source, landing, sem_shift.at[0, index], sem_shift.at[1, index]
        )

    decay_send = over_y(0, lambda peer: decay_all.at[me_y], decay_all)
    state_send = over_y(1, lambda peer: state_out.at[peer], state_in)
    back_send = over_y(2, lambda peer: back_out.at[peer], back_in)
    adj_send = over_y(3, lambda peer: adj_out.at[peer], adj_in)
    adj_back_send = over_y(4, lambda peer: adj_back_out.at[peer], adj_back_in)
    sums_y_send = over_y(5, lambda peer: sums_y.at[me_y], sums_y)
    dout_send = over_z(0, lambda peer: dout_all.at[me_z], dout_all)
    stat_send = over_z(1, lambda peer: stat_all.at[me_z], stat_all)
    proj_send = over_z(2, lambda peer: proj_out.at[peer], proj_in)
    sums_x_send = Exchange(
        "seq_0", nx, lambda peer: sums_x.at[me_x], sums_x, sem_x.at[0], sem_x.at[1]
    )
    sums_d_send = Exchange("dp", nd, lambda peer: sums_d.at[me_d], sums_d, sem_d.at[0], sem_d.at[1])
    row_sends = [shift_x(k, k + 1, row_state, row_in.at[k]) for k in range(2)]
    adj_row_sends = [shift_x(2 + k, -1 - k, adj_row, adj_row_in.at[k]) for k in range(2)]
    decay_sends = [shift_x(4, 1, row_decay, decay_in.at[0]), shift_x(5, -1, row_decay, decay_in.at[1])]

    base = (me_x * ny + me_y) * length
    loads["length"].wait()
    first = length_ref[0, 0]
    second = first + length_ref[0, 1]
    third = second + length_ref[0, 2]

    def reset_count(position):
        count = jnp.zeros(position.shape, jnp.int32)
        for start in (jnp.int32(0), first, second, third):
            here = jnp.full(position.shape, start - base, jnp.int32)
            count = count + ((here >= 0) & (here <= position)).astype(jnp.int32)
        return count

    at_row = lax.broadcasted_iota(jnp.int32, (length, length), 0)
    at_col = lax.broadcasted_iota(jnp.int32, (length, length), 1)
    count_row = reset_count(at_row)
    count_col = reset_count(at_col)
    count_heads = reset_count(lax.broadcasted_iota(jnp.int32, (length, heads), 0))
    count_end = reset_count(jnp.full((length, heads), length - 1, jnp.int32))
    not_later = (at_row >= at_col).astype(F32)
    spread = (
        lax.broadcasted_iota(jnp.int32, (heads, width), 1) // head_dim
        == lax.broadcasted_iota(jnp.int32, (heads, width), 0)
    ).astype(F32)

    loads["ld"].wait()
    loads["dt"].wait()
    dt_t = dt_ref[...]
    dt = dot((at_row == at_col).astype(F32), dt_t, 1, 1, precision=HIGH)
    running = dot(not_later, ld_ref[...], 1, 1, precision=HIGH)
    running_end = running[length - 1 :, :]
    carry_weight = jnp.where(count_heads == 0, jnp.exp(running), 0.0)
    tail_weight = jnp.where(count_heads == count_end, jnp.exp(running_end - running), 0.0)
    block_decay = jnp.where(count_end[:8] == 0, jnp.exp(jnp.broadcast_to(running_end, (8, heads))), 0.0)
    wide = dot(
        jnp.concatenate([tail_weight * dt, carry_weight, block_decay], axis=0), spread, precision=HIGH
    )
    tail_wide, carry_wide = wide[:length], wide[length : 2 * length]
    decay_all[me_y] = wide[2 * length : 2 * length + 1]
    loads["x"].wait()
    loads["b"].wait()
    x = x_ref[...].astype(F32)
    b = b_ref[...]
    fresh = dot(b, (tail_wide * x).astype(BF16), 0, 0).astype(BF16)
    fresh = fresh.reshape(ny, rows, width)
    state_out[...] = fresh
    state_in[me_y] = state_out[me_y]

    pl.semaphore_wait(barrier, (nx - 1) + (ny - 1) + (nz - 1) + (nd - 1))
    decay_send.start()
    state_send.start()
    loads["dout"].wait()
    dout_send.start()

    running_t = dot(ld_ref[...], not_later, 1, 1, precision=HIGH)
    loads["c"].wait()
    c = c_ref[...]
    same_game = count_row == count_col
    scores = jnp.where((at_row >= at_col) & same_game, dot(c, b, 1, 1), 0.0)
    scores_t = jnp.where((at_col >= at_row) & same_game, dot(b, c, 1, 1), 0.0)
    low_lane = lax.broadcasted_iota(jnp.int32, (length, lanes), 1) < head_dim

    def halves(tile):
        return jnp.concatenate([jnp.where(low_lane, tile, 0), jnp.where(low_lane, 0, tile)], axis=0)

    inside = []
    for pair in range(pairs):
        mixes, mixes_t = [], []
        for h in (2 * pair, 2 * pair + 1):
            column = jnp.broadcast_to(running[:, h : h + 1], (length, length))
            line = jnp.broadcast_to(running_t[h : h + 1], (length, length))
            mixes.append(
                (jnp.exp(jnp.minimum(column - line, 0.0)) * scores * dt_t[h : h + 1]).astype(BF16)
            )
            mixes_t.append(
                (jnp.exp(jnp.minimum(line - column, 0.0)) * scores_t * dt[:, h : h + 1]).astype(BF16)
            )
        mix_back[pair] = jnp.concatenate(mixes_t, axis=1)
        tile = x_ref[:, pair * lanes : (pair + 1) * lanes].astype(F32)
        inside.append(dot(jnp.concatenate(mixes, axis=1), halves(tile).astype(BF16)))
    inside = jnp.concatenate(inside, axis=1)
    head_of = lax.broadcasted_iota(jnp.int32, (1, width), 1) // head_dim
    skip = jnp.zeros((1, width), F32)
    loads["skip"].wait()
    for h in range(heads):
        skip = jnp.where(head_of == h, skip_ref[0, h], skip)
    inside = inside + skip * x
    loads["z"].wait()
    gate = z_ref[...].astype(F32)
    act = gate / (1.0 + jnp.exp(-gate))

    decay_send.receive_all()
    row_product = decay_all[0]
    for k in range(1, ny):
        row_product = row_product * decay_all[k]
    row_decay[...] = row_product
    for shift in decay_sends:
        shift.start()
    state_send.receive_all()
    state = state_in[0].astype(F32)
    for k in range(1, ny):
        state = decay_all[k] * state + state_in[k].astype(F32)
    row_state[...] = state.astype(BF16)
    for shift in row_sends:
        shift.start()
    loads["w"].wait()
    loads["gain"].wait()
    gain = gain_ref[...]
    for shift in decay_sends:
        shift.receive()
    for shift in row_sends:
        shift.receive()
    nearer = jnp.where(me_x >= 1, 1.0, 0.0)
    further = jnp.where(me_x >= 2, 1.0, 0.0)
    state = nearer * row_in[0].astype(F32) + further * (decay_in[0] * row_in[1].astype(F32))
    for k in range(ny):
        back_out[k] = state.astype(BF16)
        if k < ny - 1:
            state = decay_all[k] * state + state_in[k].astype(F32)
    back_in[me_y] = back_out[me_y]
    back_send.start()

    share = dout_all.shape[2]

    def columns(peer):
        return pl.ds(pl.multiple_of(peer * share, share), share)

    pulled = dot(dout_all[me_z], w_ref[:, columns(me_z)], 1, 1)
    for k in range(1, nz):
        dout_send.receive(k)
        peer = lax.rem(me_z + k, nz)
        pulled = pulled + dot(dout_all[peer], w_ref[:, columns(peer)], 1, 1)

    back_send.receive_all()
    from_left = dot(c, back_in[...].reshape(ny * rows, width))
    gated = (inside + carry_wide * from_left) * act
    normed = (gated * gain).astype(BF16)

    def over_features(values):
        part = values[:, :length]
        for k in range(1, width // length):
            part = part + values[:, k * length : (k + 1) * length]
        return jnp.sum(part.T, axis=0, keepdims=True)

    stat_all[me_z] = jnp.concatenate(
        [over_features(gated * gated), over_features(normed.astype(F32) * pulled)], axis=0
    )
    stat_send.start()
    for k in range(1, nz):
        peer = lax.rem(me_z + k, nz)
        proj_out[peer] = dot(normed, w_ref[:, columns(peer)]).astype(BF16)
        proj_send.copy(k, lambda peer: me_z).start()
    projected = dot(normed, w_ref[:, columns(me_z)])
    stat_send.receive_all()
    stats = stat_all[0]
    for k in range(1, nz):
        stats = stats + stat_all[k]
    inv_line = lax.rsqrt(stats[0:1] / total + NORM_EPS)
    pull_line = inv_line * inv_line * inv_line * stats[1:2] / total

    def down(line):
        return jnp.broadcast_to(line, (length, length)).T

    def across(tile):
        return jnp.concatenate([tile] * (width // length), axis=1)

    inv = down(inv_line)
    d_normed = across(inv) * pulled
    d_ssd = ((gain * d_normed - across(down(pull_line)) * gated) * act).astype(BF16)
    d_wide = d_ssd.astype(F32)
    adjoint = dot(c, (carry_wide * d_wide).astype(BF16), 0, 0).astype(BF16)
    adj_out[...] = adjoint.reshape(ny, rows, width)
    adj_in[me_y] = adj_out[me_y]
    adj_send.start()

    gain_part = jnp.sum(gated * d_normed, axis=0, keepdims=True)
    skip_part = jnp.sum(d_wide * x, axis=0, keepdims=True)
    fold = (
        lax.broadcasted_iota(jnp.int32, (width, length), 0) // head_dim
        == lax.broadcasted_iota(jnp.int32, (width, length), 1)
    ).astype(F32)
    skip_part = dot(jnp.broadcast_to(skip_part, (8, width)), fold, precision=HIGH)[:1]
    sums_y[me_y] = jnp.concatenate([gain_part, skip_part], axis=1)
    sums_y_send.start()

    inside_t = []
    for pair in range(pairs):
        tile = d_wide[:, pair * lanes : (pair + 1) * lanes]
        inside_t.append(dot(mix_back[pair], halves(tile).astype(BF16)))
    grad = jnp.concatenate(inside_t, axis=1) + skip * d_wide

    adj_send.receive_all()
    later = adj_in[ny - 1].astype(F32)
    for k in reversed(range(ny - 1)):
        later = decay_all[k] * later + adj_in[k].astype(F32)
    adj_row[...] = later.astype(BF16)
    for shift in adj_row_sends:
        shift.start()

    sums_y_send.receive_all()
    sums = sums_y[0]
    for k in range(1, ny):
        sums = sums + sums_y[k]
    sums_x[me_x] = sums
    sums_x_send.start()

    for shift in adj_row_sends:
        shift.receive()
    nearer = jnp.where(me_x < nx - 1, 1.0, 0.0)
    further = jnp.where(me_x < nx - 2, 1.0, 0.0)
    later = nearer * adj_row_in[0].astype(F32) + further * (decay_in[1] * adj_row_in[1].astype(F32))
    for k in reversed(range(ny)):
        adj_back_out[k] = later.astype(BF16)
        if k > 0:
            later = decay_all[k] * later + adj_in[k].astype(F32)
    adj_back_in[me_y] = adj_back_out[me_y]
    adj_back_send.start()

    sums_x_send.receive_all()
    sums = sums_x[0]
    for k in range(1, nx):
        sums = sums + sums_x[k]
    sums_d[me_d] = sums
    sums_d_send.start()

    for k in range(1, nz):
        proj_send.receive(k)
        projected = projected + proj_in[lax.rem(me_z + k, nz)].astype(F32)
    out_ref[...] = (jnp.concatenate([inv] * (share // length), axis=1) * projected).astype(BF16)

    sums_d_send.receive_all()
    sums = sums_d[0] + sums_d[1]
    gg_ref[...] = sums[:, :width]
    gs_ref[...] = sums[:, width : width + heads]

    adj_back_send.receive_all()
    right = dot(b, adj_back_in[...].reshape(ny * rows, width))
    gx_ref[...] = (grad + tail_wide * right).astype(BF16)

    for sent in (
        decay_send,
        state_send,
        back_send,
        adj_send,
        adj_back_send,
        sums_y_send,
        dout_send,
        stat_send,
        proj_send,
        sums_x_send,
        sums_d_send,
        *row_sends,
        *adj_row_sends,
        *decay_sends,
    ):
        sent.finish()


def store(*refs):
    sources, targets, sems = refs[:4], refs[4:8], refs[8]
    copies = [pltpu.make_async_copy(sources[k], targets[k], sems.at[k]) for k in range(4)]
    for copy in copies:
        copy.start()
    for copy in copies:
        copy.wait()


def mixer(
    sizes,
    ssm_input,
    gate_z,
    b_proj,
    c_proj,
    step_size,
    log_decay,
    skip_d,
    norm_gain,
    w_out,
    d_out,
    game_lengths,
):
    nx, ny, nz, nd = sizes
    length, width = ssm_input.shape[1:]
    heads = step_size.shape[2]
    state_dim = b_proj.shape[2]
    share = d_out.shape[2]
    rows = state_dim // ny
    pack = width + length

    def body(*refs):
        return kernel(nx, ny, nz, nd, *refs)

    hbm = pl.BlockSpec(memory_space=pltpu.HBM)
    smem = pl.BlockSpec(memory_space=pltpu.SMEM)
    vmem = pl.BlockSpec(memory_space=pltpu.VMEM)
    dma = pltpu.SemaphoreType.DMA
    results = pl.pallas_call(
        body,
        out_shape=(
            jax.ShapeDtypeStruct((length, share), BF16),
            jax.ShapeDtypeStruct((length, width), BF16),
            jax.ShapeDtypeStruct((1, width), F32),
            jax.ShapeDtypeStruct((1, heads), F32),
        ),
        in_specs=[hbm] * 11,
        out_specs=(vmem, vmem, vmem, vmem),
        scratch_shapes=[
            pltpu.SMEM(game_lengths.shape, jnp.int32),
            pltpu.SMEM((1, heads), F32),
            pltpu.VMEM((length, width), BF16),
            pltpu.VMEM((length, width), BF16),
            pltpu.VMEM((length, state_dim), BF16),
            pltpu.VMEM((length, state_dim), BF16),
            pltpu.VMEM((heads, length), F32),
            pltpu.VMEM((heads, length), F32),
            pltpu.VMEM((1, width), F32),
            pltpu.VMEM(w_out.shape, BF16),
            pltpu.VMEM((nz, length, share), BF16),
            pltpu.VMEM((heads // 2, length, 2 * length), BF16),
            pltpu.VMEM((ny, 1, width), F32),
            pltpu.VMEM((ny, rows, width), BF16),
            pltpu.VMEM((ny, rows, width), BF16),
            pltpu.VMEM((rows, width), BF16),
            pltpu.VMEM((2, rows, width), BF16),
            pltpu.VMEM((1, width), F32),
            pltpu.VMEM((2, 1, width), F32),
            pltpu.VMEM((ny, rows, width), BF16),
            pltpu.VMEM((ny, rows, width), BF16),
            pltpu.VMEM((ny, rows, width), BF16),
            pltpu.VMEM((ny, rows, width), BF16),
            pltpu.VMEM((rows, width), BF16),
            pltpu.VMEM((2, rows, width), BF16),
            pltpu.VMEM((ny, rows, width), BF16),
            pltpu.VMEM((ny, rows, width), BF16),
            pltpu.VMEM((nz, 2, length), F32),
            pltpu.VMEM((nz, length, share), BF16),
            pltpu.VMEM((nz, length, share), BF16),
            pltpu.VMEM((ny, 1, pack), F32),
            pltpu.VMEM((nx, 1, pack), F32),
            pltpu.VMEM((nd, 1, pack), F32),
            dma((11,)),
            dma((2, 6, ny)),
            dma((2, 3, nz)),
            dma((2, nx)),
            dma((2, nd)),
            dma((2, 6)),
        ],
        compiler_params=pltpu.CompilerParams(
            collective_id=0, has_side_effects=True, vmem_limit_bytes=VMEM_LIMIT
        ),
        name="mixer",
    )(
        *(
            pltpu.with_memory_space_constraint(array, pltpu.HBM)
            for array in (
                game_lengths,
                skip_d[None],
                ssm_input[0],
                gate_z[0],
                b_proj[0],
                c_proj[0],
                step_size[0].T,
                log_decay[0].T,
                norm_gain[None],
                w_out,
                d_out[0],
            )
        )
    )
    out, grad_x, gain_sum, skip_sum = pl.pallas_call(
        store,
        out_shape=[jax.ShapeDtypeStruct(r.shape, r.dtype) for r in results],
        in_specs=[vmem] * 4,
        out_specs=[hbm] * 4,
        scratch_shapes=[dma((4,))],
        compiler_params=pltpu.CompilerParams(vmem_limit_bytes=1 << 20),
        name="store",
    )(*results)
    return (out[None], grad_x[None], gain_sum[0], skip_sum[0])


def solution(mesh):
    nz, nd = mesh.shape["chan"], mesh.shape["dp"]
    ny = 8
    nx = mesh.shape["seq"] // ny
    finer = Mesh(mesh.devices.reshape(nx, ny, nz, nd), ("seq_0", "seq_1", "chan", "dp"))

    def local(*args):
        return mixer((nx, ny, nz, nd), *args)

    return jax.shard_map(
        local,
        mesh=finer,
        in_specs=(
            P("dp", SEQ, "chan"),
            P("dp", SEQ, "chan"),
            P("dp", SEQ, None),
            P("dp", SEQ, None),
            P("dp", SEQ, "chan"),
            P("dp", SEQ, "chan"),
            P("chan"),
            P("chan"),
            P("chan", None),
            P("dp", SEQ, "chan"),
            P("dp", None),
        ),
        out_specs=(P("dp", SEQ, "chan"), P("dp", SEQ, "chan"), P("chan"), P("chan")),
        check_vma=False,
    )
```

```python
import jax
import jax.numpy as jnp
from jax import lax
from jax.experimental import pallas as pl
from jax.experimental.pallas import tpu as pltpu
from jax.sharding import Mesh
from jax.sharding import PartitionSpec as P

SEQ = ("seq_0", "seq_1")
NORM_EPS = 1e-05
VMEM_LIMIT = 48 * 1024 * 1024
MESH = pl.DeviceIdType.MESH
HIGH = lax.Precision.HIGHEST
F32 = jnp.float32
BF16 = jnp.bfloat16


def dot(a, b, ca=1, cb=0, precision=None):
    return lax.dot_general(
        a, b, (((ca,), (cb,)), ((), ())), precision=precision, preferred_element_type=F32
    )


def by_distance(size):
    return sorted(range(1, size), key=lambda k: (-min(k, size - k), k))


class Exchange:
    def __init__(self, axis, size, source, landing, sends, receives):
        self.axis, self.size, self.me = axis, size, lax.axis_index(axis)
        self.source, self.landing = source, landing
        self.sends, self.receives = sends, receives

    def copy(self, k):
        peer = lax.rem(self.me + k, self.size)
        return pltpu.make_async_remote_copy(
            src_ref=self.source(peer),
            dst_ref=self.landing.at[self.me],
            send_sem=self.sends,
            recv_sem=self.receives,
            device_id={self.axis: peer},
            device_id_type=MESH,
        )

    def start(self):
        for k in by_distance(self.size):
            self.copy(k).start()

    def whole(self):
        most = self.landing.at[pl.ds(0, self.size - 1)]
        return pltpu.make_async_remote_copy(
            src_ref=most,
            dst_ref=most,
            send_sem=self.sends,
            recv_sem=self.receives,
            device_id={self.axis: lax.rem(self.me + 1, self.size)},
            device_id_type=MESH,
        )

    def receive_all(self):
        self.whole().wait_recv()

    def finish(self):
        self.whole().wait_send()


class Shift:
    def __init__(self, axis, size, distance, source, landing, send, receive):
        peer = lax.rem(lax.axis_index(axis) + distance + size, size)
        self.copy = pltpu.make_async_remote_copy(
            src_ref=source,
            dst_ref=landing,
            send_sem=send,
            recv_sem=receive,
            device_id={axis: peer},
            device_id_type=MESH,
        )
        self.start, self.receive, self.finish = (
            self.copy.start,
            self.copy.wait_recv,
            self.copy.wait_send,
        )


def kernel(
    nx,
    ny,
    nz,
    nd,
    length_hbm,
    skip_hbm,
    x_hbm,
    z_hbm,
    b_hbm,
    c_hbm,
    dt_hbm,
    ld_hbm,
    gain_hbm,
    w_hbm,
    dout_hbm,
    out_ref,
    gx_ref,
    gg_ref,
    gs_ref,
    length_ref,
    skip_ref,
    x_ref,
    z_ref,
    b_ref,
    c_ref,
    dt_ref,
    ld_ref,
    gain_ref,
    w_ref,
    dout_all,
    mix_back,
    decay_all,
    state_out,
    state_in,
    row_state,
    row_in,
    row_decay,
    decay_in,
    back_out,
    back_in,
    adj_out,
    adj_in,
    adj_row,
    adj_row_in,
    adj_back_out,
    adj_back_in,
    stat_all,
    proj_out,
    proj_in,
    sums_y,
    sums_x,
    sums_d,
    load_sem,
    sem_y,
    sem_z,
    sem_x,
    sem_d,
    sem_shift,
    sem_dout,
    sems_dout,
):
    length, width = x_ref.shape
    heads = dt_ref.shape[0]
    head_dim = width // heads
    pairs = heads // 2
    lanes = 2 * head_dim
    rows = state_in.shape[1]
    total = width * nz
    me_x, me_y, me_z, me_d = (lax.axis_index(a) for a in ("seq_0", "seq_1", "chan", "dp"))

    barrier = pltpu.get_barrier_semaphore()
    for axis, size, me in (
        ("seq_1", ny, me_y),
        ("chan", nz, me_z),
        ("seq_0", nx, me_x),
        ("dp", nd, me_d),
    ):
        for k in range(1, size):
            pl.semaphore_signal(
                barrier, inc=1, device_id={axis: lax.rem(me + k, size)}, device_id_type=MESH
            )

    loads = {}
    for slot, (name, source, target) in enumerate(
        (
            ("length", length_hbm, length_ref),
            ("ld", ld_hbm, ld_ref),
            ("dt", dt_hbm, dt_ref),
            ("x", x_hbm, x_ref),
            ("b", b_hbm, b_ref),
            ("dout", dout_hbm, dout_all.at[me_z]),
            ("c", c_hbm, c_ref),
            ("z", z_hbm, z_ref),
            ("gain", gain_hbm, gain_ref),
            ("skip", skip_hbm, skip_ref),
            ("w", w_hbm, w_ref),
        )
    ):
        loads[name] = pltpu.make_async_copy(source, target, load_sem.at[slot])
        loads[name].start()

    def over_y(index, source, landing):
        return Exchange("seq_1", ny, source, landing, sem_y.at[0, index], sem_y.at[1, index])

    def over_z(index, source, landing):
        return Exchange("chan", nz, source, landing, sem_z.at[0, index], sem_z.at[1, index])

    def shift_x(index, distance, source, landing):
        return Shift(
            "seq_0", nx, distance, source, landing, sem_shift.at[0, index], sem_shift.at[1, index]
        )

    decay_send = over_y(0, lambda peer: decay_all.at[me_y], decay_all)
    state_send = over_y(1, lambda peer: state_out.at[peer], state_in)
    back_send = over_y(2, lambda peer: back_out.at[peer], back_in)
    adj_send = over_y(3, lambda peer: adj_out.at[peer], adj_in)
    adj_back_send = over_y(4, lambda peer: adj_back_out.at[peer], adj_back_in)
    sums_y_send = over_y(5, lambda peer: sums_y.at[me_y], sums_y)

    def around(step):
        return lax.rem(me_z + nz + step, nz)

    def dout_copy(source, step, sem, half=None):
        piece = dout_all.at[source]
        if half is not None:
            piece = dout_all.at[source, pl.ds(half * (length // 2), length // 2)]
        return pltpu.make_async_remote_copy(
            src_ref=piece,
            dst_ref=piece,
            send_sem=sem_dout,
            recv_sem=sems_dout.at[sem],
            device_id={"chan": around(step)},
            device_id_type=MESH,
        )

    dout_sends = [dout_copy(me_z, step, me_z) for step in (2, -2, 1, -1)]
    dout_forwards = [
        dout_copy(around(-2), 2, around(-2), half=0),
        dout_copy(around(2), -2, nz, half=1),
        dout_copy(around(-2), 1, around(-2)),
        dout_copy(around(2), -1, around(2)),
    ]
    stat_send = over_z(0, lambda peer: stat_all.at[me_z], stat_all)
    proj_send = over_z(1, lambda peer: proj_out.at[peer], proj_in)
    sums_x_send = Exchange(
        "seq_0", nx, lambda peer: sums_x.at[me_x], sums_x, sem_x.at[0], sem_x.at[1]
    )
    sums_d_send = Exchange("dp", nd, lambda peer: sums_d.at[me_d], sums_d, sem_d.at[0], sem_d.at[1])
    row_sends = [shift_x(k, k + 1, row_state, row_in.at[k]) for k in range(2)]
    adj_row_sends = [shift_x(2 + k, -1 - k, adj_row, adj_row_in.at[k]) for k in range(2)]
    decay_sends = [shift_x(4, 1, row_decay, decay_in.at[0]), shift_x(5, -1, row_decay, decay_in.at[1])]

    base = (me_x * ny + me_y) * length
    loads["length"].wait()
    first = length_ref[0, 0]
    second = first + length_ref[0, 1]
    third = second + length_ref[0, 2]

    def reset_count(position):
        count = jnp.zeros(position.shape, jnp.int32)
        for start in (jnp.int32(0), first, second, third):
            here = jnp.full(position.shape, start - base, jnp.int32)
            count = count + ((here >= 0) & (here <= position)).astype(jnp.int32)
        return count

    at_row = lax.broadcasted_iota(jnp.int32, (length, length), 0)
    at_col = lax.broadcasted_iota(jnp.int32, (length, length), 1)
    count_row = reset_count(at_row)
    count_col = reset_count(at_col)
    count_heads = reset_count(lax.broadcasted_iota(jnp.int32, (length, heads), 0))
    count_end = reset_count(jnp.full((length, heads), length - 1, jnp.int32))
    not_later = (at_row >= at_col).astype(F32)
    spread = (
        lax.broadcasted_iota(jnp.int32, (heads, width), 1) // head_dim
        == lax.broadcasted_iota(jnp.int32, (heads, width), 0)
    ).astype(F32)

    loads["ld"].wait()
    loads["dt"].wait()
    dt_t = dt_ref[...]
    dt = dot((at_row == at_col).astype(F32), dt_t, 1, 1, precision=HIGH)
    running = dot(not_later, ld_ref[...], 1, 1, precision=HIGH)
    running_end = running[length - 1 :, :]
    carry_weight = jnp.where(count_heads == 0, jnp.exp(running), 0.0)
    tail_weight = jnp.where(count_heads == count_end, jnp.exp(running_end - running), 0.0)
    block_decay = jnp.where(count_end[:8] == 0, jnp.exp(jnp.broadcast_to(running_end, (8, heads))), 0.0)
    wide = dot(
        jnp.concatenate([tail_weight * dt, carry_weight, block_decay], axis=0), spread, precision=HIGH
    )
    tail_wide, carry_wide = wide[:length], wide[length : 2 * length]
    decay_all[me_y] = wide[2 * length : 2 * length + 1]
    loads["x"].wait()
    loads["b"].wait()
    x = x_ref[...].astype(F32)
    b = b_ref[...]
    fresh = dot(b, (tail_wide * x).astype(BF16), 0, 0).astype(BF16)
    fresh = fresh.reshape(ny, rows, width)
    state_out[...] = fresh
    state_in[me_y] = state_out[me_y]

    pl.semaphore_wait(barrier, (nx - 1) + (ny - 1) + (nz - 1) + (nd - 1))
    decay_send.start()
    state_send.start()
    loads["dout"].wait()
    for send in dout_sends:
        send.start()

    running_t = dot(ld_ref[...], not_later, 1, 1, precision=HIGH)
    loads["c"].wait()
    c = c_ref[...]
    same_game = count_row == count_col
    scores = jnp.where((at_row >= at_col) & same_game, dot(c, b, 1, 1), 0.0)
    scores_t = jnp.where((at_col >= at_row) & same_game, dot(b, c, 1, 1), 0.0)
    low_lane = lax.broadcasted_iota(jnp.int32, (length, lanes), 1) < head_dim

    def halves(tile):
        return jnp.concatenate([jnp.where(low_lane, tile, 0), jnp.where(low_lane, 0, tile)], axis=0)

    inside = []
    for pair in range(pairs):
        mixes, mixes_t = [], []
        for h in (2 * pair, 2 * pair + 1):
            column = jnp.broadcast_to(running[:, h : h + 1], (length, length))
            line = jnp.broadcast_to(running_t[h : h + 1], (length, length))
            mixes.append(
                (jnp.exp(jnp.minimum(column - line, 0.0)) * scores * dt_t[h : h + 1]).astype(BF16)
            )
            mixes_t.append(
                (jnp.exp(jnp.minimum(line - column, 0.0)) * scores_t * dt[:, h : h + 1]).astype(BF16)
            )
        mix_back[pair] = jnp.concatenate(mixes_t, axis=1)
        tile = x_ref[:, pair * lanes : (pair + 1) * lanes].astype(F32)
        inside.append(dot(jnp.concatenate(mixes, axis=1), halves(tile).astype(BF16)))
    inside = jnp.concatenate(inside, axis=1)
    head_of = lax.broadcasted_iota(jnp.int32, (1, width), 1) // head_dim
    skip = jnp.zeros((1, width), F32)
    loads["skip"].wait()
    for h in range(heads):
        skip = jnp.where(head_of == h, skip_ref[0, h], skip)
    inside = inside + skip * x
    loads["z"].wait()
    gate = z_ref[...].astype(F32)
    act = gate / (1.0 + jnp.exp(-gate))

    decay_send.receive_all()
    row_product = decay_all[0]
    for k in range(1, ny):
        row_product = row_product * decay_all[k]
    row_decay[...] = row_product
    for shift in decay_sends:
        shift.start()
    state_send.receive_all()
    state = state_in[0].astype(F32)
    for k in range(1, ny):
        state = decay_all[k] * state + state_in[k].astype(F32)
    row_state[...] = state.astype(BF16)
    for shift in row_sends:
        shift.start()
    for step in (-2, 2):
        dout_copy(around(step), step, around(step)).wait_recv()
    for forward in dout_forwards:
        forward.start()
    for step in (-1, 1):
        dout_copy(around(step), step, around(step)).wait_recv()
    loads["w"].wait()
    loads["gain"].wait()
    gain = gain_ref[...]
    share = dout_all.shape[2]

    def columns(peer):
        return pl.ds(pl.multiple_of(peer * share, share), share)

    def pulled_from(step):
        peer = around(step)
        return dot(dout_all[peer], w_ref[:, columns(peer)], 1, 1)

    pulled = pulled_from(0)
    for step in (-1, 1, -2, 2):
        pulled = pulled + pulled_from(step)
    for shift in decay_sends:
        shift.receive()
    for shift in row_sends:
        shift.receive()
    nearer = jnp.where(me_x >= 1, 1.0, 0.0)
    further = jnp.where(me_x >= 2, 1.0, 0.0)
    state = nearer * row_in[0].astype(F32) + further * (decay_in[0] * row_in[1].astype(F32))
    for k in range(ny):
        back_out[k] = state.astype(BF16)
        if k < ny - 1:
            state = decay_all[k] * state + state_in[k].astype(F32)
    back_in[me_y] = back_out[me_y]
    back_send.start()

    for step in (-3, 3):
        dout_copy(around(step), step, around(step)).wait_recv()
        pulled = pulled + pulled_from(step)
    dout_copy(around(4), 4, around(4), half=0).wait_recv()
    dout_copy(around(4), 4, nz, half=1).wait_recv()
    pulled = pulled + pulled_from(4)

    back_send.receive_all()
    from_left = dot(c, back_in[...].reshape(ny * rows, width))
    gated = (inside + carry_wide * from_left) * act
    normed = (gated * gain).astype(BF16)

    def over_features(values):
        part = values[:, :length]
        for k in range(1, width // length):
            part = part + values[:, k * length : (k + 1) * length]
        return jnp.sum(part.T, axis=0, keepdims=True)

    stat_all[me_z] = jnp.concatenate(
        [over_features(gated * gated), over_features(normed.astype(F32) * pulled)], axis=0
    )
    stat_send.start()
    for k in by_distance(nz):
        peer = lax.rem(me_z + k, nz)
        proj_out[peer] = dot(normed, w_ref[:, columns(peer)]).astype(BF16)
        proj_send.copy(k).start()
    projected = dot(normed, w_ref[:, columns(me_z)])
    stat_send.receive_all()
    stats = stat_all[0]
    for k in range(1, nz):
        stats = stats + stat_all[k]
    inv_line = lax.rsqrt(stats[0:1] / total + NORM_EPS)
    pull_line = inv_line * inv_line * inv_line * stats[1:2] / total

    def down(line):
        return jnp.broadcast_to(line, (length, length)).T

    def across(tile):
        return jnp.concatenate([tile] * (width // length), axis=1)

    inv = down(inv_line)
    d_normed = across(inv) * pulled
    d_ssd = ((gain * d_normed - across(down(pull_line)) * gated) * act).astype(BF16)
    d_wide = d_ssd.astype(F32)
    adjoint = dot(c, (carry_wide * d_wide).astype(BF16), 0, 0).astype(BF16)
    adj_out[...] = adjoint.reshape(ny, rows, width)
    adj_in[me_y] = adj_out[me_y]
    adj_send.start()

    gain_part = jnp.sum(gated * d_normed, axis=0, keepdims=True)
    skip_part = jnp.sum(d_wide * x, axis=0, keepdims=True)
    fold = (
        lax.broadcasted_iota(jnp.int32, (width, length), 0) // head_dim
        == lax.broadcasted_iota(jnp.int32, (width, length), 1)
    ).astype(F32)
    skip_part = dot(jnp.broadcast_to(skip_part, (8, width)), fold, precision=HIGH)[:1]
    sums_y[me_y] = jnp.concatenate([gain_part, skip_part], axis=1)
    sums_y_send.start()

    inside_t = []
    for pair in range(pairs):
        tile = d_wide[:, pair * lanes : (pair + 1) * lanes]
        inside_t.append(dot(mix_back[pair], halves(tile).astype(BF16)))
    grad = jnp.concatenate(inside_t, axis=1) + skip * d_wide

    adj_send.receive_all()
    later = adj_in[ny - 1].astype(F32)
    for k in reversed(range(ny - 1)):
        later = decay_all[k] * later + adj_in[k].astype(F32)
    adj_row[...] = later.astype(BF16)
    for shift in adj_row_sends:
        shift.start()

    for shift in adj_row_sends:
        shift.receive()
    nearer = jnp.where(me_x < nx - 1, 1.0, 0.0)
    further = jnp.where(me_x < nx - 2, 1.0, 0.0)
    later = nearer * adj_row_in[0].astype(F32) + further * (decay_in[1] * adj_row_in[1].astype(F32))
    for k in reversed(range(ny)):
        adj_back_out[k] = later.astype(BF16)
        if k > 0:
            later = decay_all[k] * later + adj_in[k].astype(F32)
    adj_back_in[me_y] = adj_back_out[me_y]
    adj_back_send.start()

    sums_y_send.receive_all()
    sums = sums_y[0]
    for k in range(1, ny):
        sums = sums + sums_y[k]
    sums_x[me_x] = sums
    sums_x_send.start()

    sums_x_send.receive_all()
    sums = sums_x[0]
    for k in range(1, nx):
        sums = sums + sums_x[k]
    sums_d[me_d] = sums
    sums_d_send.start()

    proj_send.receive_all()
    for k in range(1, nz):
        projected = projected + proj_in[lax.rem(me_z + k, nz)].astype(F32)
    out_ref[...] = (jnp.concatenate([inv] * (share // length), axis=1) * projected).astype(BF16)

    sums_d_send.receive_all()
    sums = sums_d[0] + sums_d[1]
    gg_ref[...] = sums[:, :width]
    gs_ref[...] = sums[:, width : width + heads]

    adj_back_send.receive_all()
    right = dot(b, adj_back_in[...].reshape(ny * rows, width))
    gx_ref[...] = (grad + tail_wide * right).astype(BF16)

    for sent in (
        decay_send,
        state_send,
        back_send,
        adj_send,
        adj_back_send,
        sums_y_send,
        stat_send,
        proj_send,
        sums_x_send,
        sums_d_send,
        *row_sends,
        *adj_row_sends,
        *decay_sends,
    ):
        sent.finish()
    for sent in (*dout_sends, *dout_forwards):
        sent.wait_send()


def store(*refs):
    sources, targets, sems = refs[:4], refs[4:8], refs[8]
    copies = [pltpu.make_async_copy(sources[k], targets[k], sems.at[k]) for k in range(4)]
    for copy in copies:
        copy.start()
    for copy in copies:
        copy.wait()


def mixer(
    sizes,
    ssm_input,
    gate_z,
    b_proj,
    c_proj,
    step_size,
    log_decay,
    skip_d,
    norm_gain,
    w_out,
    d_out,
    game_lengths,
):
    nx, ny, nz, nd = sizes
    length, width = ssm_input.shape[1:]
    heads = step_size.shape[2]
    state_dim = b_proj.shape[2]
    share = d_out.shape[2]
    rows = state_dim // ny
    pack = width + length

    def body(*refs):
        return kernel(nx, ny, nz, nd, *refs)

    hbm = pl.BlockSpec(memory_space=pltpu.HBM)
    smem = pl.BlockSpec(memory_space=pltpu.SMEM)
    vmem = pl.BlockSpec(memory_space=pltpu.VMEM)
    dma = pltpu.SemaphoreType.DMA
    results = pl.pallas_call(
        body,
        out_shape=(
            jax.ShapeDtypeStruct((length, share), BF16),
            jax.ShapeDtypeStruct((length, width), BF16),
            jax.ShapeDtypeStruct((1, width), F32),
            jax.ShapeDtypeStruct((1, heads), F32),
        ),
        in_specs=[hbm] * 11,
        out_specs=(vmem, vmem, vmem, vmem),
        scratch_shapes=[
            pltpu.SMEM(game_lengths.shape, jnp.int32),
            pltpu.SMEM((1, heads), F32),
            pltpu.VMEM((length, width), BF16),
            pltpu.VMEM((length, width), BF16),
            pltpu.VMEM((length, state_dim), BF16),
            pltpu.VMEM((length, state_dim), BF16),
            pltpu.VMEM((heads, length), F32),
            pltpu.VMEM((heads, length), F32),
            pltpu.VMEM((1, width), F32),
            pltpu.VMEM(w_out.shape, BF16),
            pltpu.VMEM((nz, length, share), BF16),
            pltpu.VMEM((heads // 2, length, 2 * length), BF16),
            pltpu.VMEM((ny, 1, width), F32),
            pltpu.VMEM((ny, rows, width), BF16),
            pltpu.VMEM((ny, rows, width), BF16),
            pltpu.VMEM((rows, width), BF16),
            pltpu.VMEM((2, rows, width), BF16),
            pltpu.VMEM((1, width), F32),
            pltpu.VMEM((2, 1, width), F32),
            pltpu.VMEM((ny, rows, width), BF16),
            pltpu.VMEM((ny, rows, width), BF16),
            pltpu.VMEM((ny, rows, width), BF16),
            pltpu.VMEM((ny, rows, width), BF16),
            pltpu.VMEM((rows, width), BF16),
            pltpu.VMEM((2, rows, width), BF16),
            pltpu.VMEM((ny, rows, width), BF16),
            pltpu.VMEM((ny, rows, width), BF16),
            pltpu.VMEM((nz, 2, length), F32),
            pltpu.VMEM((nz, length, share), BF16),
            pltpu.VMEM((nz, length, share), BF16),
            pltpu.VMEM((ny, 1, pack), F32),
            pltpu.VMEM((nx, 1, pack), F32),
            pltpu.VMEM((nd, 1, pack), F32),
            dma((11,)),
            dma((2, 6)),
            dma((2, 2)),
            dma((2,)),
            dma((2,)),
            dma((2, 6)),
            dma(()),
            dma((nz + 1,)),
        ],
        compiler_params=pltpu.CompilerParams(
            collective_id=0, has_side_effects=True, vmem_limit_bytes=VMEM_LIMIT
        ),
        name="mixer",
    )(
        *(
            pltpu.with_memory_space_constraint(array, pltpu.HBM)
            for array in (
                game_lengths,
                skip_d[None],
                ssm_input[0],
                gate_z[0],
                b_proj[0],
                c_proj[0],
                step_size[0].T,
                log_decay[0].T,
                norm_gain[None],
                w_out,
                d_out[0],
            )
        )
    )
    out, grad_x, gain_sum, skip_sum = pl.pallas_call(
        store,
        out_shape=[jax.ShapeDtypeStruct(r.shape, r.dtype) for r in results],
        in_specs=[vmem] * 4,
        out_specs=[hbm] * 4,
        scratch_shapes=[dma((4,))],
        compiler_params=pltpu.CompilerParams(vmem_limit_bytes=1 << 20),
        name="store",
    )(*results)
    return (out[None], grad_x[None], gain_sum[0], skip_sum[0])


def solution(mesh):
    nz, nd = mesh.shape["chan"], mesh.shape["dp"]
    ny = 8
    nx = mesh.shape["seq"] // ny
    finer = Mesh(mesh.devices.reshape(nx, ny, nz, nd), ("seq_0", "seq_1", "chan", "dp"))

    def local(*args):
        return mixer((nx, ny, nz, nd), *args)

    return jax.shard_map(
        local,
        mesh=finer,
        in_specs=(
            P("dp", SEQ, "chan"),
            P("dp", SEQ, "chan"),
            P("dp", SEQ, None),
            P("dp", SEQ, None),
            P("dp", SEQ, "chan"),
            P("dp", SEQ, "chan"),
            P("chan"),
            P("chan"),
            P("chan", None),
            P("dp", SEQ, "chan"),
            P("dp", None),
        ),
        out_specs=(P("dp", SEQ, "chan"), P("dp", SEQ, "chan"), P("chan"), P("chan")),
        check_vma=False,
    )
```
